8 devices in a mesh: batch: 1 (over z), stage: 2 (over y), seq: 4 (over x, core).
Axes of the slice: x: 2, y: 2, z: 1, core: 2. Of those that a mesh axis runs over, the one named last changes fastest.
Arguments:
- x_tokens: bfloat16 [2, 8192, 2048], P('batch', 'seq')
- norm_attn: bfloat16 [2, 2048], P('stage')
- w_query: bfloat16 [2, 2048, 1024], P('stage')
- w_key: bfloat16 [2, 2048, 1024], P('stage')
- w_value: bfloat16 [2, 2048, 2048], P('stage')
- w_gate: bfloat16 [2, 2048, 4], P('stage')
- gate_bias: float32 [2, 4], P('stage')
- norm_out: bfloat16 [2, 512], P('stage')
- w_out: bfloat16 [2, 2048, 2048], P('stage')
- norm_mlp: bfloat16 [2, 2048], P('stage')
- w_up: bfloat16 [2, 2048, 5632], P('stage')
- w_down: bfloat16 [2, 5632, 2048], P('stage')
Outputs:
- output 1: bfloat16 [2, 2, 8192, 2048], P('stage', 'batch', 'seq')
- output 2: float32 [2, 2, 4, 256, 512], P('stage', 'batch')
All inputs are finite; a program needn't handle non-finite values.
Results may differ from the reference program's by a relative error of at most 0.012754.
Values are sent between devices in bfloat16 or wider.
A program may use at most 1 GiB of HBM per device.

```python
import math
import jax
import jax.numpy as jnp
from jax import lax

NUM_SEQS = 2
CHUNK_LEN = 2048
TOKENS = 8192
MODEL_DIM = 2048
NUM_HEADS = 4
KEY_DIM = 256
VAL_DIM = 512
FFN_DIM = 5632
LAYERS = 2
NORM_EPS = 1e-6
NUM_CHUNKS = TOKENS // CHUNK_LEN
TOTAL_ROWS = NUM_SEQS * TOKENS


def dense_weight(rng_key, fan_in, fan_out):
    raw_draw = jax.random.normal(rng_key, (LAYERS, fan_in, fan_out), jnp.float32)
    return (raw_draw * fan_in ** -0.5).astype(jnp.bfloat16)


def gain_vector(rng_key, vec_width):
    raw_draw = jax.random.normal(rng_key, (LAYERS, vec_width), jnp.float32)
    return (1.0 + 0.3 * raw_draw).astype(jnp.bfloat16)


def setup_inputs(seed: int = 0, part: int = 0) -> dict:
    base_key = jax.random.key(seed)
    token_keys = jax.random.split(jax.random.fold_in(base_key, part), 2)
    weight_keys = jax.random.split(base_key, 11)
    token_noise = jax.random.normal(token_keys[0], (NUM_SEQS, TOKENS, MODEL_DIM), jnp.float32)
    walk_steps = jax.random.normal(token_keys[1], (NUM_SEQS, TOKENS, MODEL_DIM), jnp.float32)
    token_drift = jnp.cumsum(walk_steps, axis=1) * TOKENS ** -0.5
    gate_bias = math.log(CHUNK_LEN) + jax.random.uniform(weight_keys[5], (LAYERS, NUM_HEADS), jnp.float32, 0.0, 1.5)
    return {
        'x_tokens': (token_noise + 0.7 * token_drift).astype(jnp.bfloat16),
        'norm_attn': gain_vector(weight_keys[0], MODEL_DIM),
        'w_query': dense_weight(weight_keys[1], MODEL_DIM, NUM_HEADS * KEY_DIM),
        'w_key': dense_weight(weight_keys[2], MODEL_DIM, NUM_HEADS * KEY_DIM),
        'w_value': dense_weight(weight_keys[3], MODEL_DIM, NUM_HEADS * VAL_DIM),
        'w_gate': dense_weight(weight_keys[4], MODEL_DIM, NUM_HEADS),
        'gate_bias': gate_bias,
        'norm_out': gain_vector(weight_keys[6], VAL_DIM),
        'w_out': dense_weight(weight_keys[7], NUM_HEADS * VAL_DIM, MODEL_DIM),
        'norm_mlp': gain_vector(weight_keys[8], MODEL_DIM),
        'w_up': dense_weight(weight_keys[9], MODEL_DIM, FFN_DIM),
        'w_down': dense_weight(weight_keys[10], FFN_DIM, MODEL_DIM),
    }


def rms_norm(values, gain_vec):
    mean_sq = jnp.mean(values * values, axis=-1, keepdims=True)
    return values * lax.rsqrt(mean_sq + NORM_EPS) * gain_vec.astype(jnp.float32)


def chunk_step(carry_state, chunk_in):
    q_blk, k_blk, v_blk, decay_blk = chunk_in
    cum_decay = jnp.cumsum(decay_blk, axis=1)
    total_decay = cum_decay[:, -1, :]
    q_f32 = q_blk.astype(jnp.float32)
    k_f32 = k_blk.astype(jnp.float32)
    v_f32 = v_blk.astype(jnp.float32)
    inter_out = jnp.einsum('schk,shkv->schv', q_f32, carry_state) * jnp.exp(cum_decay)[..., None]
    scores = jnp.einsum('schk,sjhk->shcj', q_f32, k_f32)
    cum_heads = jnp.swapaxes(cum_decay, 1, 2)
    causal = jnp.arange(CHUNK_LEN)[:, None] >= jnp.arange(CHUNK_LEN)[None, :]
    decay_mat = jnp.exp(jnp.where(causal, cum_heads[:, :, :, None] - cum_heads[:, :, None, :], -jnp.inf))
    intra_out = jnp.einsum('shcj,sjhv->schv', scores * decay_mat, v_f32)
    k_decayed = k_f32 * jnp.exp(total_decay[:, None, :] - cum_decay)[..., None]
    new_state = jnp.exp(total_decay)[:, :, None, None] * carry_state + jnp.einsum('sjhk,sjhv->shkv', k_decayed, v_f32)
    return new_state, inter_out + intra_out


def to_chunks(values):
    shaped = values.reshape((NUM_SEQS, NUM_CHUNKS, CHUNK_LEN) + values.shape[1:])
    return jnp.moveaxis(shaped, 1, 0)


def layer_step(h_in, params):
    norm_attn, w_query, w_key, w_value, w_gate, gate_bias, norm_out, w_out, norm_mlp, w_up, w_down = params
    h_f32 = h_in.astype(jnp.float32).reshape(TOTAL_ROWS, MODEL_DIM)
    u_norm = rms_norm(h_f32, norm_attn).astype(jnp.bfloat16)
    q_all = jnp.dot(u_norm, w_query, preferred_element_type=jnp.float32).astype(jnp.bfloat16)
    k_all = (jnp.dot(u_norm, w_key, preferred_element_type=jnp.float32) * KEY_DIM ** -0.5).astype(jnp.bfloat16)
    v_all = jnp.dot(u_norm, w_value, preferred_element_type=jnp.float32).astype(jnp.bfloat16)
    log_decay = jax.nn.log_sigmoid(jnp.dot(u_norm, w_gate, preferred_element_type=jnp.float32) + gate_bias)
    chunks_in = (
        to_chunks(q_all.reshape(TOTAL_ROWS, NUM_HEADS, KEY_DIM)),
        to_chunks(k_all.reshape(TOTAL_ROWS, NUM_HEADS, KEY_DIM)),
        to_chunks(v_all.reshape(TOTAL_ROWS, NUM_HEADS, VAL_DIM)),
        to_chunks(log_decay),
    )
    zero_state = jnp.zeros((NUM_SEQS, NUM_HEADS, KEY_DIM, VAL_DIM), jnp.float32)
    final_state, chunk_outs = lax.scan(chunk_step, zero_state, chunks_in)
    attn_out = jnp.moveaxis(chunk_outs, 0, 1).reshape(TOTAL_ROWS, NUM_HEADS, VAL_DIM)
    head_norm = rms_norm(attn_out, norm_out).astype(jnp.bfloat16).reshape(TOTAL_ROWS, NUM_HEADS * VAL_DIM)
    h_mid = h_f32 + jnp.dot(head_norm, w_out, preferred_element_type=jnp.float32)
    mlp_in = rms_norm(h_mid, norm_mlp).astype(jnp.bfloat16)
    hidden = jax.nn.gelu(jnp.dot(mlp_in, w_up, preferred_element_type=jnp.float32), approximate=True).astype(jnp.bfloat16)
    h_out = (h_mid + jnp.dot(hidden, w_down, preferred_element_type=jnp.float32)).astype(jnp.bfloat16)
    h_out = h_out.reshape(NUM_SEQS, TOKENS, MODEL_DIM)
    return h_out, (h_out, final_state)


def reference(x_tokens, norm_attn, w_query, w_key, w_value, w_gate, gate_bias, norm_out, w_out, norm_mlp, w_up, w_down):
    params = (norm_attn, w_query, w_key, w_value, w_gate, gate_bias, norm_out, w_out, norm_mlp, w_up, w_down)
    last_h, (y_layers, s_final) = lax.scan(layer_step, x_tokens, params)
    return y_layers, s_final
```

```python
import functools

import jax
import jax.numpy as jnp
from jax import lax
from jax.experimental import pallas as pl
from jax.experimental.pallas import tpu as pltpu
from jax.sharding import PartitionSpec as P

NORM_EPS = 1e-6
MESH = pl.DeviceIdType.MESH
BF16 = jnp.bfloat16
F32 = jnp.float32
NUM_W = 5
NUM_W2 = 3
AHEAD = 2


def mean_sq_scale(values):
    return lax.rsqrt(jnp.mean(values * values, axis=-1, keepdims=True) + NORM_EPS)


def dot32(lhs, rhs):
    return jnp.dot(lhs, rhs, preferred_element_type=F32)


def layer_kernel(
    rows, heads, tile, tile2,
    x, wq, wk, wv, wo, w1, w2, wa, beta, g1, go, g2,
    y_out, s_out, xbuf, hbuf,
    wqkv, wbuf, w2buf, hin, u, qb, kb, vb, ob, r, hid, ybuf, state, s_in, l_own, l_recv, cum, cum_t,
    wqkv_sem, w_sem, w2_sem, hin_sem, x_send, x_recv, h_send, h_recv, y_send, y_recv, l_send_sem, l_recv_sem, s_sem, s_recv_sem,
):
    stage = lax.axis_index('stage')
    me = lax.axis_index('seq')
    chip = lax.div(me, 2)
    core = lax.rem(me, 2)
    depth = x.shape[2]
    key_dim = wq.shape[1] // heads
    val_dim = wv.shape[1] // heads
    keys = heads * key_dim
    per_home = x.shape[1] // (2 * rows)
    chunks = 4 * per_home
    q_tiles = wq.shape[1] // tile
    v_tiles = wv.shape[1] // tile
    proj_tiles = 2 * q_tiles + v_tiles
    o_tiles = depth // tile
    up_tiles = w1.shape[1] // tile
    w_tiles = o_tiles + up_tiles
    down_tiles = depth // tile2
    last = chunks - 1

    def at(stage_pos, seq_pos):
        return {'stage': stage_pos, 'seq': seq_pos}

    def span(chunk, core_pos):
        return pl.ds(pl.multiple_of((lax.rem(chunk, per_home) * 2 + core_pos) * rows, rows), rows)

    def proj_copies():
        copies = []
        for i in range(q_tiles):
            copies.append(pltpu.make_async_copy(wk.at[:, pl.ds(i * tile, tile)], wqkv.at[i], wqkv_sem.at[i]))
        for i in range(v_tiles):
            n = q_tiles + i
            copies.append(pltpu.make_async_copy(wv.at[:, pl.ds(i * tile, tile)], wqkv.at[n], wqkv_sem.at[n]))
        for i in range(q_tiles):
            n = q_tiles + v_tiles + i
            copies.append(pltpu.make_async_copy(wq.at[:, pl.ds(i * tile, tile)], wqkv.at[n], wqkv_sem.at[n]))
        return copies

    def start_w(i):
        slot = lax.rem(i, NUM_W)

        @pl.when(i < o_tiles)
        def _():
            col = pl.ds(pl.multiple_of(i * tile, tile), tile)
            pltpu.make_async_copy(wo.at[:, col], wbuf.at[slot], w_sem.at[slot]).start()

        @pl.when(i >= o_tiles)
        def _():
            col = pl.ds(pl.multiple_of((i - o_tiles) * tile, tile), tile)
            pltpu.make_async_copy(w1.at[:, col], wbuf.at[slot], w_sem.at[slot]).start()

    def wait_w(i):
        slot = lax.rem(i, NUM_W)
        pltpu.make_async_copy(w1.at[:, pl.ds(0, tile)], wbuf.at[slot], w_sem.at[slot]).wait()
        return slot

    def next_w(chunk, i):
        @pl.when((chunk < last) | (i + NUM_W < w_tiles))
        def _():
            start_w(lax.rem(i + NUM_W, w_tiles))

    def w2_copy(n, slot):
        col = pl.ds(pl.multiple_of(n * tile2, tile2), tile2)
        return pltpu.make_async_copy(w2.at[:, col], w2buf.at[slot], w2_sem.at[slot])

    def x_copy(chunk, dest):
        return pltpu.make_async_remote_copy(
            src_ref=x.at[dest // 2, span(chunk, dest % 2)],
            dst_ref=xbuf.at[chunk],
            send_sem=x_send.at[lax.rem(chunk, per_home), dest],
            recv_sem=x_recv.at[chunk],
            device_id=at(0, dest),
            device_id_type=MESH,
        )

    def x_mine(chunk, dest):
        home = lax.div(chunk, per_home)
        same = lax.div(home, 2) == dest // 2
        return (me == home) & (home != dest) & ((same & (stage == 0)) | ((lax.div(home, 2) != dest // 2) & (stage == dest % 2)))

    def push_x(chunk):
        for dest in range(4):
            @pl.when(x_mine(chunk, dest))
            def _():
                x_copy(chunk, dest).start()

    def landed(buf, sem, chunk):
        pltpu.make_async_remote_copy(
            src_ref=buf.at[chunk], dst_ref=buf.at[chunk], send_sem=x_send.at[0, 0], recv_sem=sem.at[chunk],
            device_id=at(stage, me), device_id_type=MESH,
        ).wait_recv()

    def load_h(chunk):
        slot = lax.rem(chunk, 2)
        local = me == lax.div(chunk, per_home)

        @pl.when((stage == 0) & local)
        def _():
            pltpu.make_async_copy(x.at[chip, span(chunk, core)], hin.at[slot], hin_sem.at[slot]).start()

        @pl.when((stage == 0) & (me != lax.div(chunk, per_home)))
        def _():
            landed(xbuf, x_recv, chunk)
            pltpu.make_async_copy(xbuf.at[chunk], hin.at[slot], hin_sem.at[slot]).start()

        @pl.when(stage == 1)
        def _():
            landed(hbuf, h_recv, chunk)
            pltpu.make_async_copy(hbuf.at[chunk], hin.at[slot], hin_sem.at[slot]).start()

    def h_copy(chunk):
        slot = lax.rem(chunk, 2)
        return pltpu.make_async_remote_copy(
            src_ref=ybuf.at[slot], dst_ref=hbuf.at[chunk], send_sem=h_send.at[slot], recv_sem=h_recv.at[chunk],
            device_id=at(1, me), device_id_type=MESH,
        )

    def y_local(chunk):
        slot = lax.rem(chunk, 2)
        return pltpu.make_async_copy(ybuf.at[slot], y_out.at[chip, span(chunk, core)], y_send.at[slot])

    def y_remote(chunk):
        slot = lax.rem(chunk, 2)
        return pltpu.make_async_remote_copy(
            src_ref=ybuf.at[slot], dst_ref=y_out.at[chip, span(chunk, core)], send_sem=y_send.at[slot],
            recv_sem=y_recv.at[lax.rem(chunk, per_home), me],
            device_id=at(stage, lax.div(chunk, per_home)), device_id_type=MESH,
        )

    def send_y(chunk):
        @pl.when(stage == 0)
        def _():
            h_copy(chunk).start()

        @pl.when(me == lax.div(chunk, per_home))
        def _():
            y_local(chunk).start()

        @pl.when(me != lax.div(chunk, per_home))
        def _():
            y_remote(chunk).start()

    def sent_y(chunk):
        @pl.when(stage == 0)
        def _():
            h_copy(chunk).wait_send()

        @pl.when(me == lax.div(chunk, per_home))
        def _():
            y_local(chunk).wait()

        @pl.when(me != lax.div(chunk, per_home))
        def _():
            y_remote(chunk).wait_send()

    def l_copy(chunk):
        slot = lax.rem(chunk, 2)
        return pltpu.make_async_remote_copy(
            src_ref=l_own, dst_ref=l_recv.at[slot], send_sem=l_send_sem, recv_sem=l_recv_sem.at[slot],
            device_id=at(stage, chip * 2 + 1 - core), device_id_type=MESH,
        )

    def s_local():
        return pltpu.make_async_copy(state, s_out.at[chip], s_sem.at[0])

    def s_remote():
        return pltpu.make_async_remote_copy(
            src_ref=state, dst_ref=s_out.at[chip], send_sem=s_sem.at[1], recv_sem=s_recv_sem,
            device_id=at(stage, (1 - chip) * 2 + core), device_id_type=MESH,
        )

    barrier = pltpu.get_barrier_semaphore()
    for stage_pos in range(2):
        for seq_pos in range(4):
            pl.semaphore_signal(barrier, inc=1, device_id=at(stage_pos, seq_pos), device_id_type=MESH)
    pl.semaphore_wait(barrier, 8)

    for chunk in range(AHEAD):
        push_x(jnp.int32(chunk))
    first_copies = proj_copies()
    for copy in first_copies:
        copy.start()
    for i in range(NUM_W):
        start_w(jnp.int32(i))
    for n in range(NUM_W2):
        w2_copy(n, n).start()
    state[...] = jnp.zeros_like(state)
    load_h(jnp.int32(0))
    for copy in first_copies:
        copy.wait()

    def project(i, carry):
        prod = dot32(u[...], wqkv[i])

        @pl.when(i < q_tiles)
        def _():
            scaled = (prod * key_dim ** -0.5).astype(BF16)
            kb[2 * i] = scaled[:, :key_dim]
            kb[2 * i + 1] = scaled[:, key_dim:]

        @pl.when((i >= q_tiles) & (i < q_tiles + v_tiles))
        def _():
            vb[i - q_tiles] = prod.astype(BF16)

        @pl.when(i >= q_tiles + v_tiles)
        def _():
            got = prod.astype(BF16)
            qb[2 * (i - q_tiles - v_tiles)] = got[:, :key_dim]
            qb[2 * (i - q_tiles - v_tiles) + 1] = got[:, key_dim:]

        return carry

    def chunk_body(chunk, carry):
        slot = lax.rem(chunk, 2)

        @pl.when(chunk + AHEAD < chunks)
        def _():
            push_x(chunk + AHEAD)

        pltpu.make_async_copy(hbuf.at[0], hin.at[slot], hin_sem.at[slot]).wait()
        h_f32 = hin[slot].astype(F32)
        u[...] = (h_f32 * mean_sq_scale(h_f32) * g1[...]).astype(BF16)

        gate = dot32(u[...], wa[...]) + beta[...]
        log_decay = jnp.minimum(gate, 0.0) - jnp.log1p(jnp.exp(-jnp.abs(gate)))
        row_id = lax.broadcasted_iota(jnp.int32, (rows, rows), 0)
        col_id = lax.broadcasted_iota(jnp.int32, (rows, rows), 1)
        tril = (row_id >= col_id).astype(F32)
        cum_val = jnp.dot(tril, log_decay, precision=lax.Precision.HIGHEST, preferred_element_type=F32)
        cum[...] = cum_val
        cum_t[...] = cum_val.T

        lax.fori_loop(0, q_tiles + v_tiles, project, 0)
        for h in range(heads):
            ci = cum[:, h:h + 1]
            total = cum[rows - 1:rows, h:h + 1]
            kd = (kb[h].astype(F32) * jnp.exp(total - ci)).astype(BF16)
            l_own[h * key_dim:(h + 1) * key_dim, :] = lax.dot_general(
                kd, vb[h], (((0,), (0,)), ((), ())), preferred_element_type=F32)
        last_row = cum_t[:, rows - 1:rows]
        l_own[keys:keys + 8, :] = jnp.broadcast_to(jnp.exp(last_row[:8]), (8, val_dim))
        l_copy(chunk).start()

        lax.fori_loop(q_tiles + v_tiles, proj_tiles, project, 0)
        for h in range(heads):
            ci = cum[:, h:h + 1]
            cj = cum_t[h:h + 1, :]
            scores = lax.dot_general(qb[h], kb[h], (((1,), (1,)), ((), ())), preferred_element_type=F32)
            decay = jnp.exp(jnp.where(row_id >= col_id, ci - cj, -jnp.inf))
            r[:, h * val_dim:(h + 1) * val_dim] = dot32((scores * decay).astype(BF16), vb[h])

        l_copy(chunk).wait_send()
        l_copy(chunk).wait_recv()

        def update(h, mine, theirs):
            rng = slice(h * key_dim, (h + 1) * key_dim)
            row = slice(keys + h, keys + h + 1)
            mid = state[rng] * l_recv[slot, row] + l_recv[slot, rng]
            return mid

        @pl.when(core == 0)
        def _():
            for h in range(heads):
                rng = slice(h * key_dim, (h + 1) * key_dim)
                row = slice(keys + h, keys + h + 1)
                prev = state[rng]
                s_in[rng] = prev.astype(BF16)
                mid = prev * l_own[row] + l_own[rng]
                state[rng] = mid * l_recv[slot, row] + l_recv[slot, rng]

        @pl.when(core == 1)
        def _():
            for h in range(heads):
                rng = slice(h * key_dim, (h + 1) * key_dim)
                row = slice(keys + h, keys + h + 1)
                mid = state[rng] * l_recv[slot, row] + l_recv[slot, rng]
                s_in[rng] = mid.astype(BF16)
                state[rng] = mid * l_own[row] + l_own[rng]

        @pl.when(chunk == last)
        def _():
            s_local().start()
            s_remote().start()

        for h in range(heads):
            col = slice(h * val_dim, (h + 1) * val_dim)
            inter = dot32(qb[h], s_in[h * key_dim:(h + 1) * key_dim])
            o_val = r[:, col] + inter * jnp.exp(cum[:, h:h + 1])
            ob[:, col] = (o_val * mean_sq_scale(o_val) * go[...]).astype(BF16)

        def out_proj(i, carry):
            wslot = wait_w(i)
            col = pl.ds(pl.multiple_of(i * tile, tile), tile)
            r[:, col] = hin[slot, :, col].astype(F32) + dot32(ob[...], wbuf[wslot])
            next_w(chunk, i)
            return carry

        lax.fori_loop(0, o_tiles, out_proj, 0)
        r_val = r[...]
        u[...] = (r_val * mean_sq_scale(r_val) * g2[...]).astype(BF16)

        def up(f, carry):
            i = f + o_tiles
            wslot = wait_w(i)
            for part in range(2):
                half = tile // 2
                prod = dot32(u[...], wbuf[wslot, :, part * half:(part + 1) * half])
                hid[:, pl.ds(pl.multiple_of(f * tile + part * half, half), half)] = jax.nn.gelu(prod, approximate=True).astype(BF16)
            next_w(chunk, i)
            return carry

        lax.fori_loop(0, up_tiles, up, 0)

        @pl.when(chunk >= 2)
        def _():
            sent_y(chunk - 2)

        def down(n, carry):
            g = chunk * down_tiles + n
            wslot = lax.rem(g, NUM_W2)
            w2_copy(n, wslot).wait()
            col = pl.ds(pl.multiple_of(n * tile2, tile2), tile2)
            ybuf[slot, :, col] = (r[:, col] + dot32(hid[...], w2buf[wslot])).astype(BF16)

            @pl.when((chunk < last) | (n + NUM_W2 < down_tiles))
            def _():
                w2_copy(lax.rem(n + NUM_W2, down_tiles), wslot).start()

            @pl.when((chunk < last) & (n == down_tiles - 2))
            def _():
                load_h(chunk + 1)

            return carry

        lax.fori_loop(0, down_tiles, down, 0)
        send_y(chunk)
        return carry

    lax.fori_loop(0, chunks, chunk_body, 0)

    sent_y(jnp.int32(chunks - 2))
    sent_y(jnp.int32(chunks - 1))
    s_local().wait()
    s_remote().wait_send()
    pltpu.make_async_remote_copy(
        src_ref=state, dst_ref=s_out.at[1 - chip], send_sem=s_sem.at[1], recv_sem=s_recv_sem,
        device_id=at(stage, me), device_id_type=MESH,
    ).wait_recv()

    def x_done(chunk, carry):
        for dest in range(4):
            @pl.when(x_mine(chunk, dest))
            def _():
                x_copy(chunk, dest).wait_send()
        return carry

    lax.fori_loop(0, chunks, x_done, 0)

    def y_done(e, carry):
        for src in range(4):
            @pl.when(me != src)
            def _():
                pltpu.make_async_remote_copy(
                    src_ref=ybuf.at[0], dst_ref=y_out.at[src // 2, span(e, src % 2)], send_sem=y_send.at[0],
                    recv_sem=y_recv.at[e, src], device_id=at(stage, me), device_id_type=MESH,
                ).wait_recv()
        return carry

    lax.fori_loop(0, per_home, y_done, 0)


def run_layers(rows, tile, tile2, x, wq, wk, wv, wo, w1, w2, wa, beta, g1, go, g2, heads):
    seqs, tok_len, depth = x.shape
    keys, values, ffn = wq.shape[1], wv.shape[1], w1.shape[1]
    key_dim, val_dim = keys // heads, values // heads
    per_home = tok_len // (2 * rows)
    chunks = 4 * per_home
    proj_tiles = (2 * keys + values) // tile
    hbm = pl.BlockSpec(memory_space=pl.ANY)
    vmem = pl.BlockSpec(memory_space=pltpu.VMEM)
    dma = pltpu.SemaphoreType.DMA
    outs = pl.pallas_call(
        functools.partial(layer_kernel, rows, heads, tile, tile2),
        out_shape=(
            jax.ShapeDtypeStruct((seqs, tok_len, depth), BF16),
            jax.ShapeDtypeStruct((seqs, keys, val_dim), F32),
            jax.ShapeDtypeStruct((chunks, rows, depth), BF16),
            jax.ShapeDtypeStruct((chunks, rows, depth), BF16),
        ),
        in_specs=[hbm] * 7 + [vmem] * 5,
        out_specs=(hbm, hbm, hbm, hbm),
        scratch_shapes=[
            pltpu.VMEM((proj_tiles, depth, tile), BF16),
            pltpu.VMEM((NUM_W, depth, tile), BF16),
            pltpu.VMEM((NUM_W2, ffn, tile2), BF16),
            pltpu.VMEM((2, rows, depth), BF16),
            pltpu.VMEM((rows, depth), BF16),
            pltpu.VMEM((heads, rows, key_dim), BF16),
            pltpu.VMEM((heads, rows, key_dim), BF16),
            pltpu.VMEM((heads, rows, val_dim), BF16),
            pltpu.VMEM((rows, values), BF16),
            pltpu.VMEM((rows, depth), F32),
            pltpu.VMEM((rows, ffn), BF16),
            pltpu.VMEM((2, rows, depth), BF16),
            pltpu.VMEM((keys, val_dim), F32),
            pltpu.VMEM((keys, val_dim), BF16),
            pltpu.VMEM((keys + 8, val_dim), F32),
            pltpu.VMEM((2, keys + 8, val_dim), F32),
            pltpu.VMEM((rows, 128), F32),
            pltpu.VMEM((128, rows), F32),
            dma((proj_tiles,)), dma((NUM_W,)), dma((NUM_W2,)), dma((2,)),
            dma((per_home, 4)), dma((chunks,)), dma((2,)), dma((chunks,)),
            dma((2,)), dma((per_home, 4)), dma(()), dma((2,)), dma((2,)), dma(()),
        ],
        compiler_params=pltpu.CompilerParams(
            collective_id=0, has_side_effects=True, vmem_limit_bytes=67043328),
        name='gla_layers',
    )(x, wq, wk, wv, wo, w1, w2, wa, beta, g1, go, g2)
    return outs[0], outs[1]


def solution(mesh, rows=256, tile=512, tile2=256):
    mat_spec = P('stage', None, None)
    vec_spec = P('stage', None)
    weight_specs = (vec_spec, mat_spec, mat_spec, mat_spec, mat_spec, vec_spec, vec_spec, mat_spec, vec_spec, mat_spec, mat_spec)

    def device_program(x_tokens, norm_attn, w_query, w_key, w_value, w_gate, gate_bias, norm_out, w_out, norm_mlp, w_up, w_down):
        heads = gate_bias.shape[1]
        val_dim = norm_out.shape[1]
        key_dim = w_query.shape[2] // heads
        wa = jnp.pad(w_gate[0], ((0, 0), (0, 128 - heads)))
        beta = jnp.pad(gate_bias, ((0, 0), (0, 128 - heads)))
        y, s = run_layers(
            rows, tile, tile2, x_tokens, w_query[0], w_key[0], w_value[0], w_out[0], w_up[0], w_down[0], wa, beta,
            norm_attn.astype(F32), norm_out.astype(F32), norm_mlp.astype(F32), heads)
        return y[None], s.reshape(1, x_tokens.shape[0], heads, key_dim, val_dim)

    return jax.shard_map(
        device_program,
        mesh=mesh,
        in_specs=(P('batch', 'seq', None),) + weight_specs,
        out_specs=(P('stage', 'batch', 'seq', None), P('stage', 'batch', None, None, None)),
        check_vma=False,
    )
```

```python
import functools

import jax
import jax.numpy as jnp
from jax import lax
from jax.experimental import pallas as pl
from jax.experimental.pallas import tpu as pltpu
from jax.sharding import PartitionSpec as P

NORM_EPS = 1e-6
MESH = pl.DeviceIdType.MESH
BF16 = jnp.bfloat16
F32 = jnp.float32
NUM_W = 5
NUM_W2 = 4
AHEAD = 2


def mean_sq_scale(values):
    return lax.rsqrt(jnp.mean(values * values, axis=-1, keepdims=True) + NORM_EPS)


def dot32(lhs, rhs):
    return jnp.dot(lhs, rhs, preferred_element_type=F32)


def layer_kernel(
    rows, heads, tile, tile2,
    x, wq, wk, wv, wo, w1, w2, wa, beta, g1, go, g2,
    y_out, s_out, xbuf, hbuf,
    wqkv, wbuf, w2buf, hin, u, r, hid, ybuf, state, s_in, l_own, l_recv, cum, cum_t, tril,
    wqkv_sem, w_sem, w2_sem, hin_sem, x_send, x_recv, h_send, h_recv, y_send, y_recv, l_send_sem, l_recv_sem, s_sem, s_recv_sem,
):
    stage = lax.axis_index('stage')
    me = lax.axis_index('seq')
    chip = lax.div(me, 2)
    core = lax.rem(me, 2)
    depth = x.shape[2]
    ffn = w1.shape[1]
    key_dim = wq.shape[1] // heads
    val_dim = wv.shape[1] // heads
    keys = heads * key_dim
    per_home = x.shape[1] // (2 * rows)
    chunks = 4 * per_home
    q_tiles = wq.shape[1] // tile
    v_tiles = wv.shape[1] // tile
    proj_tiles = 2 * q_tiles + v_tiles
    o_tiles = depth // tile
    up_tiles = w1.shape[1] // tile
    w_tiles = o_tiles + up_tiles
    down_tiles = depth // tile2
    last = chunks - 1

    def at(stage_pos, seq_pos):
        return {'stage': stage_pos, 'seq': seq_pos}

    def span(chunk, core_pos):
        return pl.ds(pl.multiple_of((lax.rem(chunk, per_home) * 2 + core_pos) * rows, rows), rows)

    def proj_copies():
        copies = []
        for i in range(q_tiles):
            copies.append(pltpu.make_async_copy(wk.at[:, pl.ds(i * tile, tile)], wqkv.at[i], wqkv_sem.at[i]))
        for i in range(v_tiles):
            n = q_tiles + i
            copies.append(pltpu.make_async_copy(wv.at[:, pl.ds(i * tile, tile)], wqkv.at[n], wqkv_sem.at[n]))
        for i in range(q_tiles):
            n = q_tiles + v_tiles + i
            copies.append(pltpu.make_async_copy(wq.at[:, pl.ds(i * tile, tile)], wqkv.at[n], wqkv_sem.at[n]))
        return copies

    def w_slot(chunk, i):
        if w_tiles % NUM_W == 0:
            return i % NUM_W
        return lax.rem(chunk * w_tiles + i, NUM_W)

    def start_w(i, slot):
        src = wo.at[:, pl.ds(i * tile, tile)] if i < o_tiles else w1.at[:, pl.ds((i - o_tiles) * tile, tile)]
        pltpu.make_async_copy(src, wbuf.at[slot], w_sem.at[slot]).start()

    def wait_w(chunk, i):
        slot = w_slot(chunk, i)
        pltpu.make_async_copy(w1.at[:, pl.ds(0, tile)], wbuf.at[slot], w_sem.at[slot]).wait()

    def next_w(chunk, i):
        slot = w_slot(chunk, i)
        if i + NUM_W < w_tiles:
            start_w(i + NUM_W, slot)
        else:
            @pl.when(chunk < last)
            def _():
                start_w(i + NUM_W - w_tiles, slot)

    def w2_copy(n, slot):
        return pltpu.make_async_copy(w2.at[:, pl.ds(n * tile2, tile2)], w2buf.at[slot], w2_sem.at[slot])

    def x_copy(chunk, dest):
        return pltpu.make_async_remote_copy(
            src_ref=x.at[dest // 2, span(chunk, dest % 2)],
            dst_ref=xbuf.at[chunk],
            send_sem=x_send.at[lax.rem(chunk, per_home), dest],
            recv_sem=x_recv.at[chunk],
            device_id=at(0, dest),
            device_id_type=MESH,
        )

    def x_mine(chunk, dest):
        home = lax.div(chunk, per_home)
        same = lax.div(home, 2) == dest // 2
        return (me == home) & (home != dest) & ((same & (stage == 0)) | ((lax.div(home, 2) != dest // 2) & (stage == dest % 2)))

    def push_x(chunk):
        for dest in range(4):
            @pl.when(x_mine(chunk, dest))
            def _():
                x_copy(chunk, dest).start()

    def landed(buf, sem, chunk):
        pltpu.make_async_remote_copy(
            src_ref=buf.at[chunk], dst_ref=buf.at[chunk], send_sem=x_send.at[0, 0], recv_sem=sem.at[chunk],
            device_id=at(stage, me), device_id_type=MESH,
        ).wait_recv()

    def load_h(chunk):
        slot = lax.rem(chunk, 2)
        local = me == lax.div(chunk, per_home)

        @pl.when((stage == 0) & local)
        def _():
            pltpu.make_async_copy(x.at[chip, span(chunk, core)], hin.at[slot], hin_sem.at[slot]).start()

        @pl.when((stage == 0) & (me != lax.div(chunk, per_home)))
        def _():
            landed(xbuf, x_recv, chunk)
            pltpu.make_async_copy(xbuf.at[chunk], hin.at[slot], hin_sem.at[slot]).start()

        @pl.when(stage == 1)
        def _():
            landed(hbuf, h_recv, chunk)
            pltpu.make_async_copy(hbuf.at[chunk], hin.at[slot], hin_sem.at[slot]).start()

    def part_cols(part):
        return slice(None) if part is None else pl.ds(part * 2 * tile2, 2 * tile2)

    def h_copy(chunk, part=None):
        slot = lax.rem(chunk, 2)
        return pltpu.make_async_remote_copy(
            src_ref=ybuf.at[slot, :, part_cols(part)], dst_ref=hbuf.at[chunk, :, part_cols(part)],
            send_sem=h_send.at[slot], recv_sem=h_recv.at[chunk],
            device_id=at(1, me), device_id_type=MESH,
        )

    def y_local(chunk, part=None):
        slot = lax.rem(chunk, 2)
        return pltpu.make_async_copy(
            ybuf.at[slot, :, part_cols(part)], y_out.at[chip, span(chunk, core), part_cols(part)], y_send.at[slot])

    def y_remote(chunk, part=None):
        slot = lax.rem(chunk, 2)
        return pltpu.make_async_remote_copy(
            src_ref=ybuf.at[slot, :, part_cols(part)], dst_ref=y_out.at[chip, span(chunk, core), part_cols(part)],
            send_sem=y_send.at[slot], recv_sem=y_recv.at[lax.rem(chunk, per_home), me],
            device_id=at(stage, lax.div(chunk, per_home)), device_id_type=MESH,
        )

    def send_y(chunk, part):
        @pl.when(stage == 0)
        def _():
            h_copy(chunk, part).start()

        @pl.when(me == lax.div(chunk, per_home))
        def _():
            y_local(chunk, part).start()

        @pl.when(me != lax.div(chunk, per_home))
        def _():
            y_remote(chunk, part).start()

    def sent_y(chunk):
        @pl.when(stage == 0)
        def _():
            h_copy(chunk).wait_send()

        @pl.when(me == lax.div(chunk, per_home))
        def _():
            y_local(chunk).wait()

        @pl.when(me != lax.div(chunk, per_home))
        def _():
            y_remote(chunk).wait_send()

    head_rows = key_dim + 8

    def l_copy(chunk, h):
        slot = lax.rem(chunk, 2)
        rng = pl.ds(h * head_rows, head_rows)
        return pltpu.make_async_remote_copy(
            src_ref=l_own.at[rng], dst_ref=l_recv.at[slot, rng],
            send_sem=l_send_sem.at[h], recv_sem=l_recv_sem.at[slot, h],
            device_id=at(stage, chip * 2 + 1 - core), device_id_type=MESH,
        )

    def s_rows(part):
        return pl.ds(pl.multiple_of(part * (keys // 2), keys // 2), keys // 2)

    def s_local():
        return pltpu.make_async_copy(state, s_out.at[chip], s_sem.at[0])

    def s_remote():
        return pltpu.make_async_remote_copy(
            src_ref=state.at[s_rows(core)], dst_ref=s_out.at[chip, s_rows(core)], send_sem=s_sem.at[1],
            recv_sem=s_recv_sem.at[core],
            device_id=at(stage, (1 - chip) * 2 + core), device_id_type=MESH,
        )

    def s_forward():
        part = s_out.at[1 - chip, s_rows(core)]
        return pltpu.make_async_remote_copy(
            src_ref=part, dst_ref=part, send_sem=s_sem.at[2], recv_sem=s_recv_sem.at[core],
            device_id=at(stage, chip * 2 + 1 - core), device_id_type=MESH,
        )

    def s_landed(part):
        ref = s_out.at[1 - chip, s_rows(part)]
        pltpu.make_async_remote_copy(
            src_ref=ref, dst_ref=ref, send_sem=s_sem.at[1], recv_sem=s_recv_sem.at[part],
            device_id=at(stage, me), device_id_type=MESH,
        ).wait_recv()

    barrier = pltpu.get_barrier_semaphore()
    for stage_pos in range(2):
        for seq_pos in range(4):
            pl.semaphore_signal(barrier, inc=1, device_id=at(stage_pos, seq_pos), device_id_type=MESH)
    pl.semaphore_wait(barrier, 8)

    for chunk in range(AHEAD):
        push_x(jnp.int32(chunk))
    first_copies = proj_copies()
    for copy in first_copies:
        copy.start()
    for i in range(NUM_W):
        start_w(i, i)
    for n in range(NUM_W2):
        w2_copy(n, n).start()
    state[...] = jnp.zeros_like(state)
    load_h(jnp.int32(0))
    for copy in first_copies:
        copy.wait()

    def project(n, dest, dest_col, scale):
        for part in range(2):
            half = tile // 2
            prod = dot32(u[...], wqkv[n, :, part * half:(part + 1) * half])
            if scale is not None:
                prod = prod * scale
            col = dest_col + part * half
            dest[:, col:col + half] = prod.astype(BF16)

    def norm_rows(read, gain, dest):
        step = min(16, rows)
        for i in range(rows // step):
            rng = slice(i * step, (i + 1) * step)
            vals = read(rng)
            dest[rng, :] = (vals * mean_sq_scale(vals) * gain[...]).astype(BF16)

    def q_of(h):
        return hid[:, h * key_dim:(h + 1) * key_dim]

    def k_of(h):
        return hid[:, keys + h * key_dim:keys + (h + 1) * key_dim]

    def v_of(h):
        return hid[:, 2 * keys + h * val_dim:2 * keys + (h + 1) * val_dim]

    def local_state(h):
        ci = cum[:, h:h + 1]
        total = cum[rows - 1:rows, h:h + 1]
        kd = (k_of(h).astype(F32) * jnp.exp(total - ci)).astype(BF16)
        base = h * head_rows
        l_own[base:base + key_dim, :] = lax.dot_general(
            kd, v_of(h), (((0,), (0,)), ((), ())), preferred_element_type=F32)
        l_own[base + key_dim:base + head_rows, :] = jnp.broadcast_to(jnp.exp(total), (8, val_dim))

    row_id = lax.broadcasted_iota(jnp.int32, (rows, rows), 0)
    col_id = lax.broadcasted_iota(jnp.int32, (rows, rows), 1)
    tril[...] = (row_id >= col_id).astype(F32).astype(BF16)

    def chunk_body(chunk, carry):
        slot = lax.rem(chunk, 2)

        @pl.when(chunk + AHEAD < chunks)
        def _():
            push_x(chunk + AHEAD)

        pltpu.make_async_copy(hbuf.at[0], hin.at[slot], hin_sem.at[slot]).wait()
        norm_rows(lambda rng: hin[slot, rng, :].astype(F32), g1, u)

        gate = dot32(u[...], wa[...]) + beta[...]
        log_decay = jnp.minimum(gate, 0.0) - jnp.log1p(jnp.exp(-jnp.abs(gate)))
        high = log_decay.astype(BF16)
        rest = log_decay - high.astype(F32)
        mid = rest.astype(BF16)
        low = (rest - mid.astype(F32)).astype(BF16)
        cum_val = dot32(tril[...], high) + (dot32(tril[...], mid) + dot32(tril[...], low))
        cum[...] = cum_val
        cum_t[...] = cum_val.T

        for h in range(heads):
            if h * key_dim % tile == 0:
                project(h * key_dim // tile, hid, keys + h * key_dim, key_dim ** -0.5)
            project(q_tiles + h, hid, 2 * keys + h * tile, None)
            local_state(h)
            l_copy(chunk, h).start()

        for i in range(q_tiles):
            project(q_tiles + v_tiles + i, hid, i * tile, None)
        for h in range(heads):
            ci = cum[:, h:h + 1]
            cj = cum_t[h:h + 1, :]
            scores = lax.dot_general(q_of(h), k_of(h), (((1,), (1,)), ((), ())), preferred_element_type=F32)
            decay = jnp.exp(jnp.where(row_id >= col_id, ci - cj, -jnp.inf))
            r[:, h * val_dim:(h + 1) * val_dim] = dot32((scores * decay).astype(BF16), v_of(h))

        first = core == 0

        def state_rows():
            step = min(32, key_dim)
            for h in range(heads):
                for i in range(key_dim // step):
                    sub = slice(h * key_dim + i * step, h * key_dim + (i + 1) * step)
                    lsub = slice(h * head_rows + i * step, h * head_rows + (i + 1) * step)
                    yield sub, lsub, slice(h * head_rows + key_dim, h * head_rows + key_dim + 1)

        @pl.when(core == 0)
        def _():
            for sub, lsub, row in state_rows():
                s_in[sub, :] = state[sub, :].astype(BF16)

        @pl.when(core == 1)
        def _():
            for h in range(heads):
                l_copy(chunk, h).wait_recv()
            for sub, lsub, row in state_rows():
                s_in[sub, :] = (state[sub, :] * l_recv[slot, row, :] + l_recv[slot, lsub, :]).astype(BF16)

        wait_w(chunk, 0)
        wait_w(chunk, 1)
        for h in range(heads):
            col = slice(h * val_dim, (h + 1) * val_dim)
            inter = dot32(q_of(h), s_in[h * key_dim:(h + 1) * key_dim, :])
            o_val = r[:, col] + inter * jnp.exp(cum[:, h:h + 1])
            u[:, col] = (o_val * mean_sq_scale(o_val) * go[...]).astype(BF16)

        def next_state():
            for sub, lsub, row in state_rows():
                ours = l_own[lsub, :]
                theirs = l_recv[slot, lsub, :]
                d_own = l_own[row, :]
                d_other = l_recv[slot, row, :]
                mid = state[sub, :] * jnp.where(first, d_own, d_other) + jnp.where(first, ours, theirs)
                state[sub, :] = mid * jnp.where(first, d_other, d_own) + jnp.where(first, theirs, ours)

        def out_proj(i):
            wslot = w_slot(chunk, i)
            for part in range(2):
                half = tile // 2
                col = slice(i * tile + part * half, i * tile + (part + 1) * half)
                r[:, col] = hin[slot, :, col].astype(F32) + dot32(u[...], wbuf[wslot, :, part * half:(part + 1) * half])

        for pair in range(0, o_tiles, 2):
            group = range(pair, min(pair + 2, o_tiles))
            if pair:
                for i in group:
                    wait_w(chunk, i)
            if pair + 2 >= o_tiles:
                @pl.when(core == 0)
                def _():
                    for h in range(heads):
                        l_copy(chunk, h).wait_recv()

                for h in range(heads):
                    l_copy(chunk, h).wait_send()
                next_state()
            for i in group:
                out_proj(i)
            for i in group:
                next_w(chunk, i)

        @pl.when(chunk == last)
        def _():
            s_local().start()
            s_remote().start()

        norm_rows(lambda rng: r[rng, :], g2, u)

        for pair in range(o_tiles, w_tiles, 2):
            group = range(pair, min(pair + 2, w_tiles))
            for i in group:
                wait_w(chunk, i)
            for i in group:
                wslot = w_slot(chunk, i)
                for part in range(2):
                    half = tile // 2
                    col = (i - o_tiles) * tile + part * half
                    prod = dot32(u[...], wbuf[wslot, :, part * half:(part + 1) * half])
                    hid[:, col:col + half] = jax.nn.gelu(prod, approximate=True).astype(BF16)
            for i in group:
                next_w(chunk, i)

        @pl.when(chunk >= 2)
        def _():
            sent_y(chunk - 2)

        for n in range(down_tiles):
            w2_copy(n, n % NUM_W2).wait()
            if n == down_tiles - 2:
                @pl.when(chunk < last)
                def _():
                    load_h(chunk + 1)
            col = slice(n * tile2, (n + 1) * tile2)
            ybuf[slot, :, col] = (r[:, col] + dot32(hid[:, :ffn], w2buf[n % NUM_W2])).astype(BF16)
            following = n + NUM_W2
            if following < down_tiles:
                w2_copy(following, n % NUM_W2).start()
            else:
                @pl.when(chunk < last)
                def _():
                    w2_copy(following - down_tiles, n % NUM_W2).start()
            if n % 2 == 1:
                send_y(chunk, n // 2)
        return carry

    lax.fori_loop(0, chunks, chunk_body, 0)

    s_local().wait()
    s_remote().wait_send()
    s_landed(core)
    s_forward().start()
    s_forward().wait_send()
    s_landed(1 - core)
    sent_y(jnp.int32(chunks - 2))
    sent_y(jnp.int32(chunks - 1))

    def x_done(chunk, carry):
        for dest in range(4):
            @pl.when(x_mine(chunk, dest))
            def _():
                x_copy(chunk, dest).wait_send()
        return carry

    lax.fori_loop(0, chunks, x_done, 0)

    def y_done(e, carry):
        for src in range(4):
            @pl.when(me != src)
            def _():
                pltpu.make_async_remote_copy(
                    src_ref=ybuf.at[0], dst_ref=y_out.at[src // 2, span(e, src % 2)], send_sem=y_send.at[0],
                    recv_sem=y_recv.at[e, src], device_id=at(stage, me), device_id_type=MESH,
                ).wait_recv()
        return carry

    lax.fori_loop(0, per_home, y_done, 0)


def run_layers(rows, tile, tile2, x, wq, wk, wv, wo, w1, w2, wa, beta, g1, go, g2, heads):
    seqs, tok_len, depth = x.shape
    keys, values, ffn = wq.shape[1], wv.shape[1], w1.shape[1]
    key_dim, val_dim = keys // heads, values // heads
    per_home = tok_len // (2 * rows)
    chunks = 4 * per_home
    proj_tiles = (2 * keys + values) // tile
    hbm = pl.BlockSpec(memory_space=pl.ANY)
    vmem = pl.BlockSpec(memory_space=pltpu.VMEM)
    dma = pltpu.SemaphoreType.DMA
    outs = pl.pallas_call(
        functools.partial(layer_kernel, rows, heads, tile, tile2),
        out_shape=(
            jax.ShapeDtypeStruct((seqs, tok_len, depth), BF16),
            jax.ShapeDtypeStruct((seqs, keys, val_dim), F32),
            jax.ShapeDtypeStruct((chunks, rows, depth), BF16),
            jax.ShapeDtypeStruct((chunks, rows, depth), BF16),
        ),
        in_specs=[hbm] * 7 + [vmem] * 5,
        out_specs=(hbm, hbm, hbm, hbm),
        scratch_shapes=[
            pltpu.VMEM((proj_tiles, depth, tile), BF16),
            pltpu.VMEM((NUM_W, depth, tile), BF16),
            pltpu.VMEM((NUM_W2, ffn, tile2), BF16),
            pltpu.VMEM((2, rows, depth), BF16),
            pltpu.VMEM((rows, depth), BF16),
            pltpu.VMEM((rows, depth), F32),
            pltpu.VMEM((rows, max(ffn, 2 * keys + values)), BF16),
            pltpu.VMEM((2, rows, depth), BF16),
            pltpu.VMEM((keys, val_dim), F32),
            pltpu.VMEM((keys, val_dim), BF16),
            pltpu.VMEM((keys + 8 * heads, val_dim), F32),
            pltpu.VMEM((2, keys + 8 * heads, val_dim), F32),
            pltpu.VMEM((rows, 128), F32),
            pltpu.VMEM((128, rows), F32),
            pltpu.VMEM((rows, rows), BF16),
            dma((proj_tiles,)), dma((NUM_W,)), dma((NUM_W2,)), dma((2,)),
            dma((per_home, 4)), dma((chunks,)), dma((2,)), dma((chunks,)),
            dma((2,)), dma((per_home, 4)), dma((heads,)), dma((2, heads)), dma((3,)), dma((2,)),
        ],
        compiler_params=pltpu.CompilerParams(
            collective_id=0, has_side_effects=True, vmem_limit_bytes=67043328),
        name='gla_layers',
    )(x, wq, wk, wv, wo, w1, w2, wa, beta, g1, go, g2)
    return outs[0], outs[1]


def solution(mesh, rows=256, tile=512, tile2=256):
    mat_spec = P('stage', None, None)
    vec_spec = P('stage', None)
    weight_specs = (vec_spec, mat_spec, mat_spec, mat_spec, mat_spec, vec_spec, vec_spec, mat_spec, vec_spec, mat_spec, mat_spec)

    def device_program(x_tokens, norm_attn, w_query, w_key, w_value, w_gate, gate_bias, norm_out, w_out, norm_mlp, w_up, w_down):
        heads = gate_bias.shape[1]
        val_dim = norm_out.shape[1]
        key_dim = w_query.shape[2] // heads
        wa = jnp.pad(w_gate[0], ((0, 0), (0, 128 - heads)))
        beta = jnp.pad(gate_bias, ((0, 0), (0, 128 - heads)))
        y, s = run_layers(
            rows, tile, tile2, x_tokens, w_query[0], w_key[0], w_value[0], w_out[0], w_up[0], w_down[0], wa, beta,
            norm_attn.astype(F32), norm_out.astype(F32), norm_mlp.astype(F32), heads)
        return y[None], s.reshape(1, x_tokens.shape[0], heads, key_dim, val_dim)

    return jax.shard_map(
        device_program,
        mesh=mesh,
        in_specs=(P('batch', 'seq', None),) + weight_specs,
        out_specs=(P('stage', 'batch', 'seq', None), P('stage', 'batch', None, None, None)),
        check_vma=False,
    )
```

```python
import functools

import jax
import jax.numpy as jnp
from jax import lax
from jax.experimental import pallas as pl
from jax.experimental.pallas import tpu as pltpu
from jax.sharding import PartitionSpec as P

NORM_EPS = 1e-6
MESH = pl.DeviceIdType.MESH
BF16 = jnp.bfloat16
F32 = jnp.float32
NUM_W = 5
NUM_W2 = 2
AHEAD = 2


def mean_sq_scale(values):
    return lax.rsqrt(jnp.mean(values * values, axis=-1, keepdims=True) + NORM_EPS)


def dot32(lhs, rhs):
    return jnp.dot(lhs, rhs, preferred_element_type=F32)


def layer_kernel(
    rows, heads, tile, tile2,
    x, wq, wk, wv, wo, w1, w2, wa, beta, g1, go, g2,
    y_out, s_out, xbuf, hbuf,
    wqkv, wbuf, w2buf, hin, u, r, hid, ybuf, state, s_in, l_own, l_recv, cum, cum_t, tril, raw,
    wqkv_sem, w_sem, w2_sem, hin_sem, x_send, x_recv, h_send, h_recv, y_send, y_recv, l_send_sem, l_recv_sem, s_sem, s_recv_sem,
):
    stage = lax.axis_index('stage')
    me = lax.axis_index('seq')
    chip = lax.div(me, 2)
    core = lax.rem(me, 2)
    depth = x.shape[2]
    ffn = w1.shape[1]
    key_dim = wq.shape[1] // heads
    val_dim = wv.shape[1] // heads
    keys = heads * key_dim
    per_home = x.shape[1] // (2 * rows)
    chunks = 4 * per_home
    q_tiles = wq.shape[1] // tile
    v_tiles = wv.shape[1] // tile
    proj_tiles = 2 * q_tiles + v_tiles
    o_tiles = depth // tile
    up_tiles = w1.shape[1] // tile
    w_tiles = o_tiles + up_tiles
    down_tiles = depth // tile2
    last = chunks - 1

    def at(stage_pos, seq_pos):
        return {'stage': stage_pos, 'seq': seq_pos}

    def span(chunk, core_pos):
        return pl.ds(pl.multiple_of((lax.rem(chunk, per_home) * 2 + core_pos) * rows, rows), rows)

    def proj_copies():
        copies = []
        for i in range(q_tiles):
            copies.append(pltpu.make_async_copy(wk.at[:, pl.ds(i * tile, tile)], wqkv.at[i], wqkv_sem.at[i]))
        for i in range(v_tiles):
            n = q_tiles + i
            copies.append(pltpu.make_async_copy(wv.at[:, pl.ds(i * tile, tile)], wqkv.at[n], wqkv_sem.at[n]))
        for i in range(q_tiles):
            n = q_tiles + v_tiles + i
            copies.append(pltpu.make_async_copy(wq.at[:, pl.ds(i * tile, tile)], wqkv.at[n], wqkv_sem.at[n]))
        return copies

    def w_slot(chunk, i):
        if w_tiles % NUM_W == 0:
            return i % NUM_W
        return lax.rem(chunk * w_tiles + i, NUM_W)

    def start_w(i, slot):
        src = wo.at[:, pl.ds(i * tile, tile)] if i < o_tiles else w1.at[:, pl.ds((i - o_tiles) * tile, tile)]
        pltpu.make_async_copy(src, wbuf.at[slot], w_sem.at[slot]).start()

    def wait_w(chunk, i):
        slot = w_slot(chunk, i)
        pltpu.make_async_copy(w1.at[:, pl.ds(0, tile)], wbuf.at[slot], w_sem.at[slot]).wait()

    def next_w(chunk, i):
        slot = w_slot(chunk, i)
        if i + NUM_W < w_tiles:
            start_w(i + NUM_W, slot)
        else:
            @pl.when(chunk < last)
            def _():
                start_w(i + NUM_W - w_tiles, slot)

    ffn_half = ffn // 2

    def w2_copy(n, part):
        slot = (n % NUM_W2) * 2 + part
        src = w2.at[pl.ds(part * ffn_half, ffn_half), pl.ds(n * tile2, tile2)]
        return pltpu.make_async_copy(src, w2buf.at[slot], w2_sem.at[slot])

    def x_copy(chunk, dest):
        return pltpu.make_async_remote_copy(
            src_ref=x.at[dest // 2, span(chunk, dest % 2)],
            dst_ref=xbuf.at[chunk],
            send_sem=x_send.at[lax.rem(chunk, per_home), dest],
            recv_sem=x_recv.at[chunk],
            device_id=at(0, dest),
            device_id_type=MESH,
        )

    def x_mine(chunk, dest):
        home = lax.div(chunk, per_home)
        same = lax.div(home, 2) == dest // 2
        return (me == home) & (home != dest) & ((same & (stage == 0)) | ((lax.div(home, 2) != dest // 2) & (stage == dest % 2)))

    def push_x(chunk):
        for dest in range(4):
            @pl.when(x_mine(chunk, dest))
            def _():
                x_copy(chunk, dest).start()

    def landed(buf, sem, chunk):
        pltpu.make_async_remote_copy(
            src_ref=buf.at[chunk], dst_ref=buf.at[chunk], send_sem=x_send.at[0, 0], recv_sem=sem.at[chunk],
            device_id=at(stage, me), device_id_type=MESH,
        ).wait_recv()

    def load_h(chunk):
        slot = lax.rem(chunk, 2)
        local = me == lax.div(chunk, per_home)

        @pl.when((stage == 0) & local)
        def _():
            pltpu.make_async_copy(x.at[chip, span(chunk, core)], hin.at[slot], hin_sem.at[slot]).start()

        @pl.when((stage == 0) & (me != lax.div(chunk, per_home)))
        def _():
            landed(xbuf, x_recv, chunk)
            pltpu.make_async_copy(xbuf.at[chunk], hin.at[slot], hin_sem.at[slot]).start()

        @pl.when(stage == 1)
        def _():
            landed(hbuf, h_recv, chunk)
            pltpu.make_async_copy(hbuf.at[chunk], hin.at[slot], hin_sem.at[slot]).start()

    def part_cols(part):
        return slice(None) if part is None else pl.ds(part * tile2, tile2)

    def h_copy(chunk, part=None):
        slot = lax.rem(chunk, 2)
        return pltpu.make_async_remote_copy(
            src_ref=ybuf.at[slot, :, part_cols(part)], dst_ref=hbuf.at[chunk, :, part_cols(part)],
            send_sem=h_send.at[slot], recv_sem=h_recv.at[chunk],
            device_id=at(1, me), device_id_type=MESH,
        )

    def y_local(chunk, part=None):
        slot = lax.rem(chunk, 2)
        return pltpu.make_async_copy(
            ybuf.at[slot, :, part_cols(part)], y_out.at[chip, span(chunk, core), part_cols(part)], y_send.at[slot])

    def y_remote(chunk, part=None):
        slot = lax.rem(chunk, 2)
        return pltpu.make_async_remote_copy(
            src_ref=ybuf.at[slot, :, part_cols(part)], dst_ref=y_out.at[chip, span(chunk, core), part_cols(part)],
            send_sem=y_send.at[slot], recv_sem=y_recv.at[lax.rem(chunk, per_home), me],
            device_id=at(stage, lax.div(chunk, per_home)), device_id_type=MESH,
        )

    def send_y(chunk, part):
        @pl.when(stage == 0)
        def _():
            h_copy(chunk, part).start()

        @pl.when(me == lax.div(chunk, per_home))
        def _():
            y_local(chunk, part).start()

        @pl.when(me != lax.div(chunk, per_home))
        def _():
            y_remote(chunk, part).start()

    def sent_y(chunk):
        @pl.when(stage == 0)
        def _():
            h_copy(chunk).wait_send()

        @pl.when(me == lax.div(chunk, per_home))
        def _():
            y_local(chunk).wait()

        @pl.when(me != lax.div(chunk, per_home))
        def _():
            y_remote(chunk).wait_send()

    head_rows = key_dim + 8

    def l_copy(chunk, h):
        slot = lax.rem(chunk, 2)
        rng = pl.ds(h * head_rows, head_rows)
        return pltpu.make_async_remote_copy(
            src_ref=l_own.at[rng], dst_ref=l_recv.at[slot, rng],
            send_sem=l_send_sem.at[h], recv_sem=l_recv_sem.at[slot, h],
            device_id=at(stage, chip * 2 + 1 - core), device_id_type=MESH,
        )

    def s_rows(part):
        return pl.ds(pl.multiple_of(part * (keys // 2), keys // 2), keys // 2)

    def s_local():
        return pltpu.make_async_copy(state, s_out.at[chip], s_sem.at[0])

    def s_remote():
        return pltpu.make_async_remote_copy(
            src_ref=state.at[s_rows(core)], dst_ref=s_out.at[chip, s_rows(core)], send_sem=s_sem.at[1],
            recv_sem=s_recv_sem.at[core],
            device_id=at(stage, (1 - chip) * 2 + core), device_id_type=MESH,
        )

    def s_forward():
        part = s_out.at[1 - chip, s_rows(core)]
        return pltpu.make_async_remote_copy(
            src_ref=part, dst_ref=part, send_sem=s_sem.at[2], recv_sem=s_recv_sem.at[core],
            device_id=at(stage, chip * 2 + 1 - core), device_id_type=MESH,
        )

    def s_landed(part):
        ref = s_out.at[1 - chip, s_rows(part)]
        pltpu.make_async_remote_copy(
            src_ref=ref, dst_ref=ref, send_sem=s_sem.at[1], recv_sem=s_recv_sem.at[part],
            device_id=at(stage, me), device_id_type=MESH,
        ).wait_recv()

    barrier = pltpu.get_barrier_semaphore()
    for stage_pos in range(2):
        for seq_pos in range(4):
            pl.semaphore_signal(barrier, inc=1, device_id=at(stage_pos, seq_pos), device_id_type=MESH)
    pl.semaphore_wait(barrier, 8)

    for chunk in range(AHEAD):
        push_x(jnp.int32(chunk))
    first_copies = proj_copies()
    for copy in first_copies:
        copy.start()
    for i in range(NUM_W):
        start_w(i, i)
    for n in range(NUM_W2):
        for part in range(2):
            w2_copy(n, part).start()
    state[...] = jnp.zeros_like(state)
    load_h(jnp.int32(0))
    for copy in first_copies:
        copy.wait()

    def project(n, dest, dest_col, scale):
        for part in range(2):
            half = tile // 2
            prod = dot32(u[...], wqkv[n, :, part * half:(part + 1) * half])
            if scale is not None:
                prod = prod * scale
            col = dest_col + part * half
            dest[:, col:col + half] = prod.astype(BF16)

    def norm_rows(read, gain, dest):
        step = min(16, rows)
        for i in range(rows // step):
            rng = slice(i * step, (i + 1) * step)
            vals = read(rng)
            dest[rng, :] = (vals * mean_sq_scale(vals) * gain[...]).astype(BF16)

    def q_of(h):
        return hid[:, h * key_dim:(h + 1) * key_dim]

    def k_of(h):
        return hid[:, keys + h * key_dim:keys + (h + 1) * key_dim]

    def v_of(h):
        return hid[:, 2 * keys + h * val_dim:2 * keys + (h + 1) * val_dim]

    def local_state(h):
        ci = cum[:, h:h + 1]
        total = cum[rows - 1:rows, h:h + 1]
        kd = (k_of(h).astype(F32) * jnp.exp(total - ci)).astype(BF16)
        base = h * head_rows
        l_own[base:base + key_dim, :] = lax.dot_general(
            kd, v_of(h), (((0,), (0,)), ((), ())), preferred_element_type=F32)
        l_own[base + key_dim:base + head_rows, :] = jnp.broadcast_to(jnp.exp(total), (8, val_dim))

    row_id = lax.broadcasted_iota(jnp.int32, (rows, rows), 0)
    col_id = lax.broadcasted_iota(jnp.int32, (rows, rows), 1)
    tril[...] = (row_id >= col_id).astype(F32).astype(BF16)

    def chunk_body(chunk, carry):
        slot = lax.rem(chunk, 2)

        @pl.when(chunk + AHEAD < chunks)
        def _():
            push_x(chunk + AHEAD)

        pltpu.make_async_copy(hbuf.at[0], hin.at[slot], hin_sem.at[slot]).wait()
        norm_rows(lambda rng: hin[slot, rng, :].astype(F32), g1, u)

        gate = dot32(u[...], wa[...]) + beta[...]
        log_decay = jnp.minimum(gate, 0.0) - jnp.log1p(jnp.exp(-jnp.abs(gate)))
        high = log_decay.astype(BF16)
        rest = log_decay - high.astype(F32)
        mid = rest.astype(BF16)
        low = (rest - mid.astype(F32)).astype(BF16)
        cum_val = dot32(tril[...], high) + (dot32(tril[...], mid) + dot32(tril[...], low))
        cum[...] = cum_val
        cum_t[...] = cum_val.T

        project(0, hid, keys, key_dim ** -0.5)
        project(q_tiles, hid, 2 * keys, None)
        for h in range(heads):
            if h + 1 < heads:
                if (h + 1) * key_dim % tile == 0:
                    n = (h + 1) * key_dim // tile
                    project(n, hid, keys + n * tile, key_dim ** -0.5)
                project(q_tiles + h + 1, hid, 2 * keys + (h + 1) * tile, None)
            else:
                for i in range(q_tiles):
                    project(q_tiles + v_tiles + i, hid, i * tile, None)
            local_state(h)
            l_copy(chunk, h).start()

        for h in range(heads):
            ci = cum[:, h:h + 1]
            cj = cum_t[h:h + 1, :]
            scores = lax.dot_general(q_of(h), k_of(h), (((1,), (1,)), ((), ())), preferred_element_type=F32)
            decay = jnp.exp(jnp.where(row_id >= col_id, ci - cj, -jnp.inf))
            r[:, h * val_dim:(h + 1) * val_dim] = dot32((scores * decay).astype(BF16), v_of(h))

        first = core == 0

        def state_rows(these=range(heads)):
            step = min(32, key_dim)
            for h in these:
                for i in range(key_dim // step):
                    sub = slice(h * key_dim + i * step, h * key_dim + (i + 1) * step)
                    lsub = slice(h * head_rows + i * step, h * head_rows + (i + 1) * step)
                    yield sub, lsub, slice(h * head_rows + key_dim, h * head_rows + key_dim + 1)

        @pl.when(core == 0)
        def _():
            for sub, lsub, row in state_rows():
                s_in[sub, :] = state[sub, :].astype(BF16)

        @pl.when(core == 1)
        def _():
            for h in range(heads):
                l_copy(chunk, h).wait_recv()
            for sub, lsub, row in state_rows():
                s_in[sub, :] = (state[sub, :] * l_recv[slot, row, :] + l_recv[slot, lsub, :]).astype(BF16)

        wait_w(chunk, 0)
        wait_w(chunk, 1)
        for h in range(heads):
            col = slice(h * val_dim, (h + 1) * val_dim)
            inter = dot32(q_of(h), s_in[h * key_dim:(h + 1) * key_dim, :])
            o_val = r[:, col] + inter * jnp.exp(cum[:, h:h + 1])
            u[:, col] = (o_val * mean_sq_scale(o_val) * go[...]).astype(BF16)

        def next_state(h):
            for sub, lsub, row in state_rows((h,)):
                ours = l_own[lsub, :]
                theirs = l_recv[slot, lsub, :]
                d_own = l_own[row, :]
                d_other = l_recv[slot, row, :]
                mid = state[sub, :] * jnp.where(first, d_own, d_other) + jnp.where(first, ours, theirs)
                state[sub, :] = mid * jnp.where(first, d_other, d_own) + jnp.where(first, theirs, ours)

        def out_proj(i):
            wslot = w_slot(chunk, i)
            for part in range(2):
                half = tile // 2
                col = slice(i * tile + part * half, i * tile + (part + 1) * half)
                r[:, col] = hin[slot, :, col].astype(F32) + dot32(u[...], wbuf[wslot, :, part * half:(part + 1) * half])

        for pair in range(0, o_tiles, 2):
            group = range(pair, min(pair + 2, o_tiles))
            if pair:
                for i in group:
                    wait_w(chunk, i)
            for i in group:
                out_proj(i)
            for i in group:
                next_w(chunk, i)

        @pl.when(core == 0)
        def _():
            for h in range(heads):
                l_copy(chunk, h).wait_recv()

        for h in range(heads):
            l_copy(chunk, h).wait_send()
        norm_rows(lambda rng: r[rng, :], g2, u)

        half = tile // 2
        staged = None
        for pair in range(o_tiles, w_tiles, 2):
            group = range(pair, min(pair + 2, w_tiles))
            for i in group:
                wait_w(chunk, i)
            if staged is not None:
                hid[:, staged:staged + half] = jax.nn.gelu(raw[...], approximate=True).astype(BF16)
            for i in group:
                wslot = w_slot(chunk, i)
                for part in range(2):
                    col = (i - o_tiles) * tile + part * half
                    prod = dot32(u[...], wbuf[wslot, :, part * half:(part + 1) * half])
                    if i == group[-1] and part == 1 and i + 1 < w_tiles:
                        raw[...] = prod
                        staged = col
                    else:
                        hid[:, col:col + half] = jax.nn.gelu(prod, approximate=True).astype(BF16)
            h = (pair - o_tiles) // 2
            if h < heads:
                next_state(h)
            for i in group:
                next_w(chunk, i)

        @pl.when(chunk == last)
        def _():
            s_local().start()
            s_remote().start()

        @pl.when(chunk >= 2)
        def _():
            sent_y(chunk - 2)

        for n in range(down_tiles):
            for part in range(2):
                w2_copy(n, part).wait()
            if n == down_tiles - 1:
                @pl.when(chunk < last)
                def _():
                    load_h(chunk + 1)
            col = slice(n * tile2, (n + 1) * tile2)
            wslot = (n % NUM_W2) * 2
            front = dot32(hid[:, :ffn_half], w2buf[wslot])
            following = n + NUM_W2
            if following < down_tiles:
                w2_copy(following, 0).start()
            else:
                @pl.when(chunk < last)
                def _():
                    w2_copy(following - down_tiles, 0).start()
            back = dot32(hid[:, ffn_half:ffn], w2buf[wslot + 1])
            ybuf[slot, :, col] = (r[:, col] + (front + back)).astype(BF16)
            if following < down_tiles:
                w2_copy(following, 1).start()
            else:
                @pl.when(chunk < last)
                def _():
                    w2_copy(following - down_tiles, 1).start()
            send_y(chunk, n)
        return carry

    lax.fori_loop(0, chunks, chunk_body, 0)

    s_local().wait()
    s_remote().wait_send()
    s_landed(core)
    s_forward().start()
    s_forward().wait_send()
    s_landed(1 - core)
    sent_y(jnp.int32(chunks - 2))
    sent_y(jnp.int32(chunks - 1))

    def x_done(chunk, carry):
        for dest in range(4):
            @pl.when(x_mine(chunk, dest))
            def _():
                x_copy(chunk, dest).wait_send()
        return carry

    lax.fori_loop(0, chunks, x_done, 0)

    def y_done(e, carry):
        for src in range(4):
            @pl.when(me != src)
            def _():
                pltpu.make_async_remote_copy(
                    src_ref=ybuf.at[0], dst_ref=y_out.at[src // 2, span(e, src % 2)], send_sem=y_send.at[0],
                    recv_sem=y_recv.at[e, src], device_id=at(stage, me), device_id_type=MESH,
                ).wait_recv()
        return carry

    lax.fori_loop(0, per_home, y_done, 0)


def run_layers(rows, tile, tile2, x, wq, wk, wv, wo, w1, w2, wa, beta, g1, go, g2, heads):
    seqs, tok_len, depth = x.shape
    keys, values, ffn = wq.shape[1], wv.shape[1], w1.shape[1]
    key_dim, val_dim = keys // heads, values // heads
    per_home = tok_len // (2 * rows)
    chunks = 4 * per_home
    proj_tiles = (2 * keys + values) // tile
    hbm = pl.BlockSpec(memory_space=pl.ANY)
    vmem = pl.BlockSpec(memory_space=pltpu.VMEM)
    dma = pltpu.SemaphoreType.DMA
    outs = pl.pallas_call(
        functools.partial(layer_kernel, rows, heads, tile, tile2),
        out_shape=(
            jax.ShapeDtypeStruct((seqs, tok_len, depth), BF16),
            jax.ShapeDtypeStruct((seqs, keys, val_dim), F32),
            jax.ShapeDtypeStruct((chunks, rows, depth), BF16),
            jax.ShapeDtypeStruct((chunks, rows, depth), BF16),
        ),
        in_specs=[hbm] * 7 + [vmem] * 5,
        out_specs=(hbm, hbm, hbm, hbm),
        scratch_shapes=[
            pltpu.VMEM((proj_tiles, depth, tile), BF16),
            pltpu.VMEM((NUM_W, depth, tile), BF16),
            pltpu.VMEM((2 * NUM_W2, ffn // 2, tile2), BF16),
            pltpu.VMEM((2, rows, depth), BF16),
            pltpu.VMEM((rows, depth), BF16),
            pltpu.VMEM((rows, depth), F32),
            pltpu.VMEM((rows, max(ffn, 2 * keys + values)), BF16),
            pltpu.VMEM((2, rows, depth), BF16),
            pltpu.VMEM((keys, val_dim), F32),
            pltpu.VMEM((keys, val_dim), BF16),
            pltpu.VMEM((keys + 8 * heads, val_dim), F32),
            pltpu.VMEM((2, keys + 8 * heads, val_dim), F32),
            pltpu.VMEM((rows, 128), F32),
            pltpu.VMEM((128, rows), F32),
            pltpu.VMEM((rows, rows), BF16),
            pltpu.VMEM((rows, tile // 2), F32),
            dma((proj_tiles,)), dma((NUM_W,)), dma((2 * NUM_W2,)), dma((2,)),
            dma((per_home, 4)), dma((chunks,)), dma((2,)), dma((chunks,)),
            dma((2,)), dma((per_home, 4)), dma((heads,)), dma((2, heads)), dma((3,)), dma((2,)),
        ],
        compiler_params=pltpu.CompilerParams(
            collective_id=0, has_side_effects=True, vmem_limit_bytes=67043328),
        name='gla_layers',
    )(x, wq, wk, wv, wo, w1, w2, wa, beta, g1, go, g2)
    return outs[0], outs[1]


def solution(mesh, rows=256, tile=512, tile2=512):
    mat_spec = P('stage', None, None)
    vec_spec = P('stage', None)
    weight_specs = (vec_spec, mat_spec, mat_spec, mat_spec, mat_spec, vec_spec, vec_spec, mat_spec, vec_spec, mat_spec, mat_spec)

    def device_program(x_tokens, norm_attn, w_query, w_key, w_value, w_gate, gate_bias, norm_out, w_out, norm_mlp, w_up, w_down):
        heads = gate_bias.shape[1]
        val_dim = norm_out.shape[1]
        key_dim = w_query.shape[2] // heads
        wa = jnp.pad(w_gate[0], ((0, 0), (0, 128 - heads)))
        beta = jnp.pad(gate_bias, ((0, 0), (0, 128 - heads)))
        y, s = run_layers(
            rows, tile, tile2, x_tokens, w_query[0], w_key[0], w_value[0], w_out[0], w_up[0], w_down[0], wa, beta,
            norm_attn.astype(F32), norm_out.astype(F32), norm_mlp.astype(F32), heads)
        return y[None], s.reshape(1, x_tokens.shape[0], heads, key_dim, val_dim)

    return jax.shard_map(
        device_program,
        mesh=mesh,
        in_specs=(P('batch', 'seq', None),) + weight_specs,
        out_specs=(P('stage', 'batch', 'seq', None), P('stage', 'batch', None, None, None)),
        check_vma=False,
    )
```

```python
import functools

import jax
import jax.numpy as jnp
from jax import lax
from jax.experimental import pallas as pl
from jax.experimental.pallas import tpu as pltpu
from jax.sharding import PartitionSpec as P

NORM_EPS = 1e-6
MESH = pl.DeviceIdType.MESH
BF16 = jnp.bfloat16
F32 = jnp.float32
NUM_W = 5
NUM_W2 = 2
AHEAD = 2


def mean_sq_scale(values):
    return lax.rsqrt(jnp.mean(values * values, axis=-1, keepdims=True) + NORM_EPS)


def dot32(lhs, rhs):
    return jnp.dot(lhs, rhs, preferred_element_type=F32)


def layer_kernel(
    rows, heads, tile, tile2,
    x, wq, wk, wv, wo, w1, w2, wa_in, beta_in, g1_in, go_in, g2_in,
    y_out, s_out, xbuf, hbuf,
    wqkv, wbuf, w2buf, hin, u, r, hid, ybuf, state, s_in, l_own, l_recv, cum, cum_t, tril, raw, wa, beta, g1, go, g2,
    wqkv_sem, w_sem, w2_sem, hin_sem, x_send, x_recv, h_send, h_recv, y_send, y_recv, l_send_sem, l_recv_sem, s_sem, s_recv_sem,
):
    stage = lax.axis_index('stage')
    me = lax.axis_index('seq')
    chip = lax.div(me, 2)
    core = lax.rem(me, 2)
    depth = x.shape[2]
    ffn = w1.shape[1]
    key_dim = wq.shape[1] // heads
    val_dim = wv.shape[1] // heads
    keys = heads * key_dim
    per_home = x.shape[1] // (2 * rows)
    chunks = 4 * per_home
    q_tiles = wq.shape[1] // tile
    v_tiles = wv.shape[1] // tile
    proj_tiles = 2 * q_tiles + v_tiles
    o_tiles = depth // tile
    up_tiles = w1.shape[1] // tile
    w_tiles = o_tiles + up_tiles
    down_tiles = depth // tile2
    last = chunks - 1

    def at(stage_pos, seq_pos):
        return {'stage': stage_pos, 'seq': seq_pos}

    def span(chunk, core_pos):
        return pl.ds(pl.multiple_of((lax.rem(chunk, per_home) * 2 + core_pos) * rows, rows), rows)

    def proj_copies():
        copies = []
        for i in range(q_tiles):
            copies.append(pltpu.make_async_copy(wk.at[:, pl.ds(i * tile, tile)], wqkv.at[i], wqkv_sem.at[i]))
        for i in range(v_tiles):
            n = q_tiles + i
            copies.append(pltpu.make_async_copy(wv.at[:, pl.ds(i * tile, tile)], wqkv.at[n], wqkv_sem.at[n]))
        for i in range(q_tiles):
            n = q_tiles + v_tiles + i
            copies.append(pltpu.make_async_copy(wq.at[:, pl.ds(i * tile, tile)], wqkv.at[n], wqkv_sem.at[n]))
        return copies

    def w_slot(chunk, i):
        if w_tiles % NUM_W == 0:
            return i % NUM_W
        return lax.rem(chunk * w_tiles + i, NUM_W)

    def start_w(i, slot):
        src = wo.at[:, pl.ds(i * tile, tile)] if i < o_tiles else w1.at[:, pl.ds((i - o_tiles) * tile, tile)]
        pltpu.make_async_copy(src, wbuf.at[slot], w_sem.at[slot]).start()

    def wait_w(chunk, i):
        slot = w_slot(chunk, i)
        pltpu.make_async_copy(w1.at[:, pl.ds(0, tile)], wbuf.at[slot], w_sem.at[slot]).wait()

    def next_w(chunk, i):
        slot = w_slot(chunk, i)
        if i + NUM_W < w_tiles:
            start_w(i + NUM_W, slot)
        else:
            @pl.when(chunk < last)
            def _():
                start_w(i + NUM_W - w_tiles, slot)

    ffn_half = ffn // 2

    def w2_copy(n, part):
        slot = (n % NUM_W2) * 2 + part
        src = w2.at[pl.ds(part * ffn_half, ffn_half), pl.ds(n * tile2, tile2)]
        return pltpu.make_async_copy(src, w2buf.at[slot], w2_sem.at[slot])

    def x_copy(chunk, dest):
        return pltpu.make_async_remote_copy(
            src_ref=x.at[dest // 2, span(chunk, dest % 2)],
            dst_ref=xbuf.at[chunk],
            send_sem=x_send.at[lax.rem(chunk, per_home), dest],
            recv_sem=x_recv.at[chunk],
            device_id=at(0, dest),
            device_id_type=MESH,
        )

    def x_mine(chunk, dest):
        home = lax.div(chunk, per_home)
        same = lax.div(home, 2) == dest // 2
        return (me == home) & (home != dest) & ((same & (stage == 0)) | ((lax.div(home, 2) != dest // 2) & (stage == dest % 2)))

    def push_x(chunk):
        for dest in range(4):
            @pl.when(x_mine(chunk, dest))
            def _():
                x_copy(chunk, dest).start()

    def landed(buf, sem, chunk):
        pltpu.make_async_remote_copy(
            src_ref=buf.at[chunk], dst_ref=buf.at[chunk], send_sem=x_send.at[0, 0], recv_sem=sem.at[chunk],
            device_id=at(stage, me), device_id_type=MESH,
        ).wait_recv()

    def load_h(chunk):
        slot = lax.rem(chunk, 2)
        local = me == lax.div(chunk, per_home)

        @pl.when((stage == 0) & local)
        def _():
            pltpu.make_async_copy(x.at[chip, span(chunk, core)], hin.at[slot], hin_sem.at[slot]).start()

        @pl.when((stage == 0) & (me != lax.div(chunk, per_home)))
        def _():
            landed(xbuf, x_recv, chunk)
            pltpu.make_async_copy(xbuf.at[chunk], hin.at[slot], hin_sem.at[slot]).start()

        @pl.when(stage == 1)
        def _():
            landed(hbuf, h_recv, chunk)
            pltpu.make_async_copy(hbuf.at[chunk], hin.at[slot], hin_sem.at[slot]).start()

    def part_cols(part):
        return slice(None) if part is None else pl.ds(part * tile2, tile2)

    def h_copy(chunk, part=None):
        slot = lax.rem(chunk, 2)
        return pltpu.make_async_remote_copy(
            src_ref=ybuf.at[slot, :, part_cols(part)], dst_ref=hbuf.at[chunk, :, part_cols(part)],
            send_sem=h_send.at[slot], recv_sem=h_recv.at[chunk],
            device_id=at(1, me), device_id_type=MESH,
        )

    def y_local(chunk, part=None):
        slot = lax.rem(chunk, 2)
        return pltpu.make_async_copy(
            ybuf.at[slot, :, part_cols(part)], y_out.at[chip, span(chunk, core), part_cols(part)], y_send.at[slot])

    def y_remote(chunk, part=None):
        slot = lax.rem(chunk, 2)
        return pltpu.make_async_remote_copy(
            src_ref=ybuf.at[slot, :, part_cols(part)], dst_ref=y_out.at[chip, span(chunk, core), part_cols(part)],
            send_sem=y_send.at[slot], recv_sem=y_recv.at[lax.rem(chunk, per_home), me],
            device_id=at(stage, lax.div(chunk, per_home)), device_id_type=MESH,
        )

    def send_y(chunk, part):
        @pl.when(stage == 0)
        def _():
            h_copy(chunk, part).start()

        @pl.when(me == lax.div(chunk, per_home))
        def _():
            y_local(chunk, part).start()

        @pl.when(me != lax.div(chunk, per_home))
        def _():
            y_remote(chunk, part).start()

    def sent_y(chunk):
        @pl.when(stage == 0)
        def _():
            h_copy(chunk).wait_send()

        @pl.when(me == lax.div(chunk, per_home))
        def _():
            y_local(chunk).wait()

        @pl.when(me != lax.div(chunk, per_home))
        def _():
            y_remote(chunk).wait_send()

    head_rows = key_dim + 8

    def l_copy(chunk, part):
        slot = lax.rem(chunk, 2)
        rng = pl.ds(part * (heads // 2) * head_rows, (heads // 2) * head_rows)
        return pltpu.make_async_remote_copy(
            src_ref=l_own.at[rng], dst_ref=l_recv.at[slot, rng],
            send_sem=l_send_sem.at[part], recv_sem=l_recv_sem.at[slot, part],
            device_id=at(stage, chip * 2 + 1 - core), device_id_type=MESH,
        )

    def s_rows(part):
        return pl.ds(pl.multiple_of(part * (keys // 2), keys // 2), keys // 2)

    def s_local():
        return pltpu.make_async_copy(state, s_out.at[chip], s_sem.at[0])

    def s_remote():
        return pltpu.make_async_remote_copy(
            src_ref=state.at[s_rows(core)], dst_ref=s_out.at[chip, s_rows(core)], send_sem=s_sem.at[1],
            recv_sem=s_recv_sem.at[core],
            device_id=at(stage, (1 - chip) * 2 + core), device_id_type=MESH,
        )

    def s_forward():
        part = s_out.at[1 - chip, s_rows(core)]
        return pltpu.make_async_remote_copy(
            src_ref=part, dst_ref=part, send_sem=s_sem.at[2], recv_sem=s_recv_sem.at[core],
            device_id=at(stage, chip * 2 + 1 - core), device_id_type=MESH,
        )

    def s_landed(part):
        ref = s_out.at[1 - chip, s_rows(part)]
        pltpu.make_async_remote_copy(
            src_ref=ref, dst_ref=ref, send_sem=s_sem.at[1], recv_sem=s_recv_sem.at[part],
            device_id=at(stage, me), device_id_type=MESH,
        ).wait_recv()

    barrier = pltpu.get_barrier_semaphore()
    for stage_pos in range(2):
        for seq_pos in range(4):
            pl.semaphore_signal(barrier, inc=1, device_id=at(stage_pos, seq_pos), device_id_type=MESH)
    pl.semaphore_wait(barrier, 8)

    for chunk in range(AHEAD):
        push_x(jnp.int32(chunk))
    first_copies = proj_copies()
    for copy in first_copies:
        copy.start()
    for i in range(NUM_W):
        start_w(i, i)
    for n in range(NUM_W2):
        for part in range(2):
            w2_copy(n, part).start()
    load_h(jnp.int32(0))
    state[...] = jnp.zeros_like(state)
    g1[...] = g1_in[...].astype(F32)
    go[...] = go_in[...].astype(F32)
    g2[...] = g2_in[...].astype(F32)
    beta[...] = jnp.zeros_like(beta)
    beta[:, :heads] = beta_in[...]
    lanes = wa.shape[1]
    l_own[:lanes, :] = jnp.zeros((lanes, val_dim), F32)
    for i in range(depth // val_dim):
        l_own[:heads, :] = wa_in[:, i * val_dim:(i + 1) * val_dim].astype(F32)
        wa[i * val_dim:(i + 1) * val_dim, :] = l_own[:lanes, :].T.astype(BF16)
    for copy in first_copies:
        copy.wait()

    def project(n, dest, dest_col, scale):
        for part in range(2):
            half = tile // 2
            prod = dot32(u[...], wqkv[n, :, part * half:(part + 1) * half])
            if scale is not None:
                prod = prod * scale
            col = dest_col + part * half
            dest[:, col:col + half] = prod.astype(BF16)

    def norm_rows(read, gain, dest):
        step = min(16, rows)
        for i in range(rows // step):
            rng = slice(i * step, (i + 1) * step)
            vals = read(rng)
            dest[rng, :] = (vals * mean_sq_scale(vals) * gain[...]).astype(BF16)

    def q_of(h):
        return hid[:, h * key_dim:(h + 1) * key_dim]

    def k_of(h):
        return hid[:, keys + h * key_dim:keys + (h + 1) * key_dim]

    def v_of(h):
        return hid[:, 2 * keys + h * val_dim:2 * keys + (h + 1) * val_dim]

    def local_state(h):
        ci = cum[:, h:h + 1]
        total = cum[rows - 1:rows, h:h + 1]
        kd = (k_of(h).astype(F32) * jnp.exp(total - ci)).astype(BF16)
        base = h * head_rows
        l_own[base:base + key_dim, :] = lax.dot_general(
            kd, v_of(h), (((0,), (0,)), ((), ())), preferred_element_type=F32)
        l_own[base + key_dim:base + head_rows, :] = jnp.broadcast_to(jnp.exp(total), (8, val_dim))

    row_id = lax.broadcasted_iota(jnp.int32, (rows, rows), 0)
    col_id = lax.broadcasted_iota(jnp.int32, (rows, rows), 1)
    tril[...] = (row_id >= col_id).astype(F32).astype(BF16)

    def chunk_body(chunk, carry):
        slot = lax.rem(chunk, 2)

        @pl.when(chunk + AHEAD < chunks)
        def _():
            push_x(chunk + AHEAD)

        pltpu.make_async_copy(hbuf.at[0], hin.at[slot], hin_sem.at[slot]).wait()
        norm_rows(lambda rng: hin[slot, rng, :].astype(F32), g1, u)

        gate = dot32(u[...], wa[...]) + beta[...]
        log_decay = jnp.minimum(gate, 0.0) - jnp.log1p(jnp.exp(-jnp.abs(gate)))
        high = log_decay.astype(BF16)
        rest = log_decay - high.astype(F32)
        mid = rest.astype(BF16)
        low = (rest - mid.astype(F32)).astype(BF16)
        cum_val = dot32(tril[...], high) + (dot32(tril[...], mid) + dot32(tril[...], low))
        cum[...] = cum_val
        cum_t[...] = cum_val.T

        heads_half = heads // 2
        for i in range(q_tiles):
            project(i, hid, keys + i * tile, key_dim ** -0.5)
        for i in range(v_tiles - 1):
            project(q_tiles + i, hid, 2 * keys + i * tile, None)
        for h in range(heads_half):
            local_state(h)
        l_copy(chunk, 0).start()
        project(q_tiles + v_tiles - 1, hid, 2 * keys + (v_tiles - 1) * tile, None)
        for i in range(q_tiles):
            project(q_tiles + v_tiles + i, hid, i * tile, None)
        for h in range(heads_half, heads):
            local_state(h)
        l_copy(chunk, 1).start()

        first = core == 0

        def state_rows(these=range(heads)):
            step = min(32, key_dim)
            for h in these:
                for i in range(key_dim // step):
                    sub = slice(h * key_dim + i * step, h * key_dim + (i + 1) * step)
                    lsub = slice(h * head_rows + i * step, h * head_rows + (i + 1) * step)
                    yield sub, lsub, slice(h * head_rows + key_dim, h * head_rows + key_dim + 1)

        @pl.when(core == 0)
        def _():
            for sub, lsub, row in state_rows():
                s_in[sub, :] = state[sub, :].astype(BF16)

        @pl.when(core == 1)
        def _():
            for part in range(2):
                l_copy(chunk, part).wait_recv()
            for sub, lsub, row in state_rows():
                s_in[sub, :] = (state[sub, :] * l_recv[slot, row, :] + l_recv[slot, lsub, :]).astype(BF16)

        wait_w(chunk, 0)
        wait_w(chunk, 1)
        for h in range(heads):
            ci = cum[:, h:h + 1]
            cj = cum_t[h:h + 1, :]
            scores = lax.dot_general(q_of(h), k_of(h), (((1,), (1,)), ((), ())), preferred_element_type=F32)
            decay = jnp.exp(jnp.where(row_id >= col_id, ci - cj, -jnp.inf))
            r[:, h * val_dim:(h + 1) * val_dim] = dot32((scores * decay).astype(BF16), v_of(h))

        for h in range(heads):
            col = slice(h * val_dim, (h + 1) * val_dim)
            inter = dot32(q_of(h), s_in[h * key_dim:(h + 1) * key_dim, :])
            o_val = r[:, col] + inter * jnp.exp(cum[:, h:h + 1])
            u[:, col] = (o_val * mean_sq_scale(o_val) * go[...]).astype(BF16)

        def next_state(h):
            for sub, lsub, row in state_rows((h,)):
                ours = l_own[lsub, :]
                theirs = l_recv[slot, lsub, :]
                d_own = l_own[row, :]
                d_other = l_recv[slot, row, :]
                mid = state[sub, :] * jnp.where(first, d_own, d_other) + jnp.where(first, ours, theirs)
                state[sub, :] = mid * jnp.where(first, d_other, d_own) + jnp.where(first, theirs, ours)

        def out_proj(i):
            wslot = w_slot(chunk, i)
            for part in range(2):
                half = tile // 2
                col = slice(i * tile + part * half, i * tile + (part + 1) * half)
                r[:, col] = hin[slot, :, col].astype(F32) + dot32(u[...], wbuf[wslot, :, part * half:(part + 1) * half])

        for pair in range(0, o_tiles, 2):
            group = range(pair, min(pair + 2, o_tiles))
            if pair:
                for i in group:
                    wait_w(chunk, i)
            for i in group:
                out_proj(i)
            for i in group:
                next_w(chunk, i)

        norm_rows(lambda rng: r[rng, :], g2, u)

        half = tile // 2
        staged = None
        for pair in range(o_tiles, w_tiles, 2):
            group = range(pair, min(pair + 2, w_tiles))
            h = (pair - o_tiles) // 2 - 1
            if h == 0:
                @pl.when(core == 0)
                def _():
                    for part in range(2):
                        l_copy(chunk, part).wait_recv()

                for part in range(2):
                    l_copy(chunk, part).wait_send()
            for i in group:
                wait_w(chunk, i)
            if staged is not None:
                hid[:, staged:staged + half] = jax.nn.gelu(raw[...], approximate=True).astype(BF16)
            for i in group:
                wslot = w_slot(chunk, i)
                for part in range(2):
                    col = (i - o_tiles) * tile + part * half
                    prod = dot32(u[...], wbuf[wslot, :, part * half:(part + 1) * half])
                    if i == group[-1] and part == 1 and i + 1 < w_tiles:
                        raw[...] = prod
                        staged = col
                    else:
                        hid[:, col:col + half] = jax.nn.gelu(prod, approximate=True).astype(BF16)
            if 0 <= h < heads:
                next_state(h)
            for i in group:
                next_w(chunk, i)

        @pl.when(chunk == last)
        def _():
            s_local().start()
            s_remote().start()

        @pl.when(chunk >= 2)
        def _():
            sent_y(chunk - 2)

        for n in range(down_tiles):
            for part in range(2):
                w2_copy(n, part).wait()
            if n == down_tiles - 1:
                @pl.when(chunk < last)
                def _():
                    load_h(chunk + 1)
            col = slice(n * tile2, (n + 1) * tile2)
            wslot = (n % NUM_W2) * 2
            front = dot32(hid[:, :ffn_half], w2buf[wslot])
            following = n + NUM_W2
            if following < down_tiles:
                w2_copy(following, 0).start()
            else:
                @pl.when(chunk < last)
                def _():
                    w2_copy(following - down_tiles, 0).start()
            back = dot32(hid[:, ffn_half:ffn], w2buf[wslot + 1])
            ybuf[slot, :, col] = (r[:, col] + (front + back)).astype(BF16)
            if following < down_tiles:
                w2_copy(following, 1).start()
            else:
                @pl.when(chunk < last)
                def _():
                    w2_copy(following - down_tiles, 1).start()
            send_y(chunk, n)
        return carry

    lax.fori_loop(0, chunks, chunk_body, 0)

    s_local().wait()
    s_remote().wait_send()
    s_landed(core)
    s_forward().start()
    s_forward().wait_send()
    s_landed(1 - core)
    sent_y(jnp.int32(chunks - 2))
    sent_y(jnp.int32(chunks - 1))

    def x_done(chunk, carry):
        for dest in range(4):
            @pl.when(x_mine(chunk, dest))
            def _():
                x_copy(chunk, dest).wait_send()
        return carry

    lax.fori_loop(0, chunks, x_done, 0)

    def y_done(e, carry):
        for src in range(4):
            @pl.when(me != src)
            def _():
                pltpu.make_async_remote_copy(
                    src_ref=ybuf.at[0], dst_ref=y_out.at[src // 2, span(e, src % 2)], send_sem=y_send.at[0],
                    recv_sem=y_recv.at[e, src], device_id=at(stage, me), device_id_type=MESH,
                ).wait_recv()
        return carry

    lax.fori_loop(0, per_home, y_done, 0)


def run_layers(rows, tile, tile2, x, wq, wk, wv, wo, w1, w2, wa, beta, g1, go, g2, heads):
    seqs, tok_len, depth = x.shape
    keys, values, ffn = wq.shape[1], wv.shape[1], w1.shape[1]
    key_dim, val_dim = keys // heads, values // heads
    per_home = tok_len // (2 * rows)
    chunks = 4 * per_home
    proj_tiles = (2 * keys + values) // tile
    hbm = pl.BlockSpec(memory_space=pl.ANY)
    vmem = pl.BlockSpec(memory_space=pltpu.VMEM)
    dma = pltpu.SemaphoreType.DMA
    outs = pl.pallas_call(
        functools.partial(layer_kernel, rows, heads, tile, tile2),
        out_shape=(
            jax.ShapeDtypeStruct((seqs, tok_len, depth), BF16),
            jax.ShapeDtypeStruct((seqs, keys, val_dim), F32),
            jax.ShapeDtypeStruct((chunks, rows, depth), BF16),
            jax.ShapeDtypeStruct((chunks, rows, depth), BF16),
        ),
        in_specs=[hbm] * 7 + [vmem] * 5,
        out_specs=(hbm, hbm, hbm, hbm),
        scratch_shapes=[
            pltpu.VMEM((proj_tiles, depth, tile), BF16),
            pltpu.VMEM((NUM_W, depth, tile), BF16),
            pltpu.VMEM((2 * NUM_W2, ffn // 2, tile2), BF16),
            pltpu.VMEM((2, rows, depth), BF16),
            pltpu.VMEM((rows, depth), BF16),
            pltpu.VMEM((rows, depth), F32),
            pltpu.VMEM((rows, max(ffn, 2 * keys + values)), BF16),
            pltpu.VMEM((2, rows, depth), BF16),
            pltpu.VMEM((keys, val_dim), F32),
            pltpu.VMEM((keys, val_dim), BF16),
            pltpu.VMEM((keys + 8 * heads, val_dim), F32),
            pltpu.VMEM((2, keys + 8 * heads, val_dim), F32),
            pltpu.VMEM((rows, 128), F32),
            pltpu.VMEM((128, rows), F32),
            pltpu.VMEM((rows, rows), BF16),
            pltpu.VMEM((rows, tile // 2), F32),
            pltpu.VMEM((depth, 128), BF16),
            pltpu.VMEM((1, 128), F32),
            pltpu.VMEM((1, depth), F32),
            pltpu.VMEM((1, val_dim), F32),
            pltpu.VMEM((1, depth), F32),
            dma((proj_tiles,)), dma((NUM_W,)), dma((2 * NUM_W2,)), dma((2,)),
            dma((per_home, 4)), dma((chunks,)), dma((2,)), dma((chunks,)),
            dma((2,)), dma((per_home, 4)), dma((2,)), dma((2, 2)), dma((3,)), dma((2,)),
        ],
        compiler_params=pltpu.CompilerParams(
            collective_id=0, has_side_effects=True, vmem_limit_bytes=67043328),
        name='gla_layers',
    )(x, wq, wk, wv, wo, w1, w2, wa, beta, g1, go, g2)
    return outs[0], outs[1]


def solution(mesh, rows=256, tile=512, tile2=512):
    mat_spec = P('stage', None, None)
    vec_spec = P('stage', None)
    weight_specs = (vec_spec, mat_spec, mat_spec, mat_spec, mat_spec, vec_spec, vec_spec, mat_spec, vec_spec, mat_spec, mat_spec)

    def device_program(x_tokens, norm_attn, w_query, w_key, w_value, w_gate, gate_bias, norm_out, w_out, norm_mlp, w_up, w_down):
        heads = gate_bias.shape[1]
        val_dim = norm_out.shape[1]
        key_dim = w_query.shape[2] // heads
        y, s = run_layers(
            rows, tile, tile2, x_tokens, w_query[0], w_key[0], w_value[0], w_out[0], w_up[0], w_down[0], w_gate[0].T, gate_bias,
            norm_attn, norm_out, norm_mlp, heads)
        return y[None], s.reshape(1, x_tokens.shape[0], heads, key_dim, val_dim)

    return jax.shard_map(
        device_program,
        mesh=mesh,
        in_specs=(P('batch', 'seq', None),) + weight_specs,
        out_specs=(P('stage', 'batch', 'seq', None), P('stage', 'batch', None, None, None)),
        check_vma=False,
    )
```
